16 devices in a mesh: dp: 2 (over y, z), tp: 8 (over x, core).
Axes of the slice: x: 4, y: 2, z: 1, core: 2. Of those that a mesh axis runs over, the one named last changes fastest.
The devices are a block of a 4x4x8 slice.
Arguments:
- x: bfloat16 [4096, 5120], P(('dp', 'tp')), parts along dimension 0
- dy: bfloat16 [4096, 5120], P(('dp', 'tp')), parts along dimension 0
- gain: bfloat16 [5120], replicated
- wq: bfloat16 [5120, 5120], P(None, 'tp')
- wk: bfloat16 [5120, 5120], P(None, 'tp')
- wv: bfloat16 [5120, 5120], P(None, 'tp')
- wo: bfloat16 [5120, 5120], P('tp')
Outputs:
- output 1: bfloat16 [4096, 5120], P(('dp', 'tp')), parts along dimension 0
- output 2: float32 [2, 5120], P('dp'), parts along dimension 0
- output 3: bfloat16 [10240, 5120], P('dp', 'tp'), parts along dimension 0
- output 4: bfloat16 [10240, 5120], P('dp', 'tp'), parts along dimension 0
- output 5: bfloat16 [10240, 5120], P('dp', 'tp'), parts along dimension 0
- output 6: bfloat16 [10240, 5120], P(('dp', 'tp')), parts along dimension 0
There are 2 independent parts. The reference program is written for one: setup_inputs(seed, part) draws one part's arguments, and reference() takes and returns one part's arrays. A program takes and returns all parts, laid end to end along the dimension named above; an argument that names none is the same for every part.
All inputs are finite; a program needn't handle non-finite values.
Results may differ from the reference program's by a relative error of at most 0.018.
Values are sent between devices in bfloat16 or wider.
A program may use at most 768 MiB of HBM per device.

```python
import jax
import jax.numpy as jnp
from jax import lax

ROWS = 2048
D = 5120
HEADS = 40
KV_HEADS = 40
HEAD = 128
THETA = 10000


def setup_inputs(seed: int = 0, part: int = 0) -> dict:
    kx, ky, kn, kq, kk, kv, ko = jax.random.split(jax.random.key(seed), 7)

    def weights(key, rows, columns):
        return jax.random.normal(key, (rows, columns), jnp.float32) * rows**-0.5

    drawn = {
        "x": jax.random.normal(jax.random.fold_in(kx, part), (ROWS, D), jnp.float32),
        "dy": jax.random.normal(jax.random.fold_in(ky, part), (ROWS, D), jnp.float32) * ROWS**-0.5,
        "gain": 1 + 0.1 * jax.random.normal(kn, (D,), jnp.float32),
        "wq": 2 * weights(kq, D, HEADS * HEAD),
        "wk": 2 * weights(kk, D, KV_HEADS * HEAD),
        "wv": 4 * weights(kv, D, KV_HEADS * HEAD),
        "wo": weights(ko, HEADS * HEAD, D),
    }
    return {k: v.astype(jnp.bfloat16) for k, v in drawn.items()}


def normed(x, gain):
    wide = x.astype(jnp.float32)
    scale = lax.rsqrt(jnp.mean(wide * wide, -1, keepdims=True) + 1e-6)
    return (wide * scale * gain.astype(jnp.float32)).astype(jnp.bfloat16)


def turned(t, place, theta):
    half = t.shape[-1] // 2
    angle = place.astype(jnp.float32)[:, None] * theta ** (-jnp.arange(half, dtype=jnp.float32) / half)
    cos, sin = jnp.cos(angle)[:, None], jnp.sin(angle)[:, None]
    a, b = t[..., :half].astype(jnp.float32), t[..., half:].astype(jnp.float32)
    return jnp.concatenate([a * cos - b * sin, b * cos + a * sin], -1).astype(jnp.bfloat16)


def matmul(a, w):
    return jnp.dot(a, w, preferred_element_type=jnp.float32).astype(jnp.bfloat16)


def einsum(form, a, b):
    return jnp.einsum(form, a.astype(jnp.float32), b.astype(jnp.float32))


def attention(q, k, v):
    scores = einsum("tgsd,ugd->gstu", q, k) * q.shape[-1] ** -0.5
    token = jnp.arange(q.shape[0])
    scores = jnp.where(token[:, None] >= token, scores, -jnp.inf)
    weights = jax.nn.softmax(scores, -1).astype(jnp.bfloat16)
    return einsum("gstu,ugd->tgsd", weights, v).astype(jnp.bfloat16)


def forward(x, gain, wq, wk, wv, wo):
    rows = x.shape[0]
    a, place = normed(x, gain), jnp.arange(rows)
    k = turned(matmul(a, wk).reshape(rows, -1, HEAD), place, THETA)
    q = turned(matmul(a, wq).reshape(rows, -1, HEAD), place, THETA).reshape(rows, k.shape[1], -1, HEAD)
    v = matmul(a, wv).reshape(rows, -1, HEAD)
    seen = attention(q, k, v).reshape(rows, -1)
    return (x.astype(jnp.float32) + jnp.dot(seen, wo, preferred_element_type=jnp.float32)).astype(jnp.bfloat16)


def reference(x, dy, gain, wq, wk, wv, wo):
    _, back = jax.vjp(forward, x, gain.astype(jnp.float32), wq, wk, wv, wo)
    by_x, by_gain, *by_weights = back(dy)
    return (by_x, by_gain[None], *by_weights)
```

```python
import functools

import jax
import jax.numpy as jnp
import numpy as np
from jax import lax
from jax.experimental import pallas as pl
from jax.experimental.pallas import tpu as pltpu
from jax.sharding import PartitionSpec as P

NEG = -1e30
HIDDEN = 2 * NEG
LOG2E = 1.4426950408889634
HEAD = 128
THETA = 10000
MOST = 64 * 2**20 - 64 * 1024
MESH = pl.DeviceIdType.MESH


def _dot(a, b, ca, cb):
    return lax.dot_general(a, b, (((ca,), (cb,)), ((), ())), preferred_element_type=jnp.float32)


def _gap(bq):
    return lax.broadcasted_iota(jnp.int32, (bq, bq), 1) - lax.broadcasted_iota(jnp.int32, (bq, bq), 0)


def _spread(turn):
    left = lax.broadcasted_iota(jnp.int32, turn.shape, 1) < HEAD // 2
    other = pltpu.roll(turn, HEAD // 2, 1)
    return jnp.where(left, turn, other), jnp.where(left, -other, turn)


def _backward(q_ref, k_ref, v_ref, do_ref, lse_ref, delta_ref, turn_ref, dq_ref, dk_ref, dv_ref, dq_s, dk_s, dv_s, gap_s):
    heads, bq, _ = q_ref.shape
    iq = pl.program_id(0)
    scale = HEAD**-0.5
    e = scale * LOG2E

    @pl.when(iq == 0)
    def _():
        gap_s[...] = _gap(bq)
        dk_s[...] = jnp.zeros_like(dk_s)
        dv_s[...] = jnp.zeros_like(dv_s)

    dq_s[...] = jnp.zeros_like(dq_s)
    lses = [lse_ref[h] * LOG2E for h in range(heads)]
    deltas = [delta_ref[h] for h in range(heads)]

    def block(j, masked):
        here = pl.ds(pl.multiple_of(j * bq, bq), bq)
        scores = [_dot(k_ref[h, here, :], q_ref[h], 1, 1) for h in range(heads)]
        dps = [_dot(v_ref[h, here, :], do_ref[h], 1, 1) for h in range(heads)]
        for h in range(heads):
            p = jnp.exp2(scores[h] * e - lses[h])
            if masked:
                p = jnp.where(gap_s[...] >= 0, p, 0.0)
            ds = (p * (dps[h] - deltas[h])).astype(jnp.bfloat16)
            dv_s[h, here, :] += _dot(p.astype(jnp.bfloat16), do_ref[h], 1, 0)
            dk_s[h, here, :] += _dot(ds, q_ref[h], 1, 0)
            dq_s[h] += _dot(k_ref[h, here, :].T, ds, 1, 0)

    lax.fori_loop(0, iq, lambda j, _: block(j, False), None)
    block(iq, True)

    def back(g, cos, sin):
        g = g.astype(jnp.bfloat16).astype(jnp.float32)
        return (g * cos - pltpu.roll(g, HEAD // 2, 1) * sin).astype(jnp.bfloat16)

    cos, sin = _spread(turn_ref[pl.ds(pl.multiple_of(iq * bq, bq), bq), :])
    for h in range(heads):
        dq_ref[:, h * HEAD : (h + 1) * HEAD] = back((dq_s[h] * scale).T, cos, sin)

    @pl.when(iq == pl.num_programs(0) - 1)
    def _():
        def rows(r, _):
            at = pl.ds(pl.multiple_of(r * bq, bq), bq)
            cos, sin = _spread(turn_ref[at, :])
            for h in range(heads):
                lanes = slice(h * HEAD, (h + 1) * HEAD)
                dk_ref[at, lanes] = back(dk_s[h, at, :] * scale, cos, sin)
                dv_ref[at, lanes] = dv_s[h, at, :].astype(jnp.bfloat16)

        lax.fori_loop(0, pl.num_programs(0), rows, None)


def attend_bwd(q, k, v, d_out, lse, delta, bq):
    heads, whole, _ = q.shape
    blocks = pl.BlockSpec((heads, bq, HEAD), lambda i: (0, i, 0))
    full = pl.BlockSpec((heads, whole, HEAD), lambda i: (0, 0, 0))
    stat = pl.BlockSpec((heads, 1, bq), lambda i: (0, 0, i))
    flat = jax.ShapeDtypeStruct((whole, heads * HEAD), jnp.bfloat16)
    all_rows = pl.BlockSpec(flat.shape, lambda i: (0, 0))
    return pl.pallas_call(
        _backward,
        grid=(whole // bq,),
        in_specs=[blocks, full, full, blocks, stat, stat, pl.BlockSpec((whole, HEAD), lambda i: (0, 0))],
        out_specs=[pl.BlockSpec((bq, heads * HEAD), lambda i: (i, 0)), all_rows, all_rows],
        out_shape=[flat] * 3,
        scratch_shapes=[pltpu.VMEM((heads, HEAD, bq), jnp.float32), pltpu.VMEM((heads, whole, HEAD), jnp.float32),
                        pltpu.VMEM((heads, whole, HEAD), jnp.float32), pltpu.VMEM((bq, bq), jnp.int32)],
        compiler_params=pltpu.CompilerParams(dimension_semantics=("arbitrary",), vmem_limit_bytes=MOST),
        cost_estimate=pl.CostEstimate(flops=5 * heads * whole * whole * HEAD, transcendentals=heads * whole * whole, bytes_accessed=14 * q.size),
        name="attend_bwd",
    )(q, k, v, d_out, lse, delta, _table(whole))


FIRST = ((0, 4, "right"), (1, 5, "left"), (0, 2, "partner"), (1, 3, "partner"), (1, 8, "right"), (0, 9, "left"))
THEN = {2: ((4, 12, "right"), (5, 13, "left"), (4, 6, "partner"), (5, 7, "partner")), 4: ((8, 10, "partner"), (9, 11, "partner")),
        6: ((12, 14, "partner"), (13, 15, "partner"))}
UNITS = 8


def _peers(n):
    me = lax.axis_index("tp")
    partner = me + 1 - 2 * lax.rem(me, 2)
    return me, {"right": lax.rem(me + 2, n), "left": lax.rem(me + n - 2, n), "partner": partner}


def _greet(peers):
    barrier = pltpu.get_barrier_semaphore()
    for who in peers.values():
        pl.semaphore_signal(barrier, inc=1, device_id={"tp": who}, device_id_type=MESH)
    return lambda: pl.semaphore_wait(barrier, len(peers))


def _rows_of(u, me, n, half):
    s = u // 2
    base = me + (u % 2) * (1 - 2 * (me % 2))
    mid, far = (s * (3 - s)) // 2, s // 3
    a = (base + n - 2 * mid + (n // 2) * far) % n
    b = (base + 2 * mid + (n // 2) * far) % n
    h = s // 2 - far
    return pl.multiple_of((2 * a + h) * half, half), pl.multiple_of((2 * b + 1 - h) * half, half)


def _hop(buf, send, recv, peers, half, src, dst, whom):
    return pltpu.make_async_remote_copy(src_ref=buf.at[pl.ds(src * half, half)], dst_ref=buf.at[pl.ds(dst * half, half)],
                                        send_sem=send.at[dst], recv_sem=recv.at[dst], device_id={"tp": peers[whom]}, device_id_type=MESH)


def _arrive(u, hop):
    hops = [h for h in FIRST] + [h for hs in THEN.values() for h in hs]
    for k in range(1, UNITS):
        @pl.when(u == k)
        def _():
            for src, dst, whom in hops:
                if dst // 2 == k:
                    hop(src, dst, whom).wait_recv()
            for h in THEN.get(k, ()):
                hop(*h).start()


def _sent(hop):
    for h in FIRST + sum(THEN.values(), ()):
        hop(*h).wait_send()


def _project(n, heads, x_ref, gain_ref, turn_ref, wq_ref, wk_ref, wv_ref, all_ref, q_ref, k_ref, v_ref, buf, w_s, o_s, send, recv, w_sem,
             all_sem, o_sem):
    rows, d = x_ref.shape
    half, wide = rows // 2, heads * HEAD
    me, peers = _peers(n)
    ready = _greet(peers)
    loads = [pltpu.make_async_copy(w, w_s.at[:, pl.ds(i * wide, wide)], w_sem.at[i]) for i, w in enumerate((wq_ref, wk_ref, wv_ref))]
    for load in loads:
        load.start()
    gain = gain_ref[...].astype(jnp.float32)

    def norm(i, _):
        at = pl.ds(pl.multiple_of(i * 16, 16), 16)
        t = x_ref[at, :].astype(jnp.float32)
        scale = lax.rsqrt(jnp.mean(t * t, -1, keepdims=True) + 1e-6)
        buf[at, :] = (t * scale * gain).astype(jnp.bfloat16)

    lax.fori_loop(0, rows // 16, norm, None)
    ready()
    hop = functools.partial(_hop, buf, send, recv, peers, half)
    for h in FIRST:
        hop(*h).start()
    for load in loads:
        load.wait()

    def keep(u):
        return [pltpu.make_async_copy(buf.at[pl.ds(u * rows + i * half, half)], all_ref.at[pl.ds(at, half)], all_sem.at[u, i])
                for i, at in enumerate(_rows_of(u, me, n, half))]

    def out(u):
        return [pltpu.make_async_copy(o_s.at[u, pl.ds(m * heads, heads), pl.ds(i * half, half)], ref.at[:, pl.ds(at, half)],
                                      o_sem.at[u, i, m])
                for i, at in enumerate(_rows_of(u, me, n, half)) for m, ref in enumerate((q_ref, k_ref, v_ref))]

    def unit(u, _):
        _arrive(u, hop)
        for copy in keep(u):
            copy.start()
        a, b = _rows_of(u, me, n, half)
        cos, sin = _spread(jnp.concatenate([turn_ref[pl.ds(a, half), :], turn_ref[pl.ds(b, half), :]], axis=0))

        def tile(j, _):
            t = jnp.dot(buf[pl.ds(pl.multiple_of(u * rows, rows), rows), :], w_s[:, pl.ds(pl.multiple_of(j * 2 * HEAD, 2 * HEAD), 2 * HEAD)],
                        preferred_element_type=jnp.float32).astype(jnp.bfloat16)
            for i in range(2):
                one = t[:, i * HEAD : (i + 1) * HEAD].astype(jnp.float32)
                straight = 2 * j + i >= 2 * heads
                c, s = jnp.where(straight, 1.0, cos), jnp.where(straight, 0.0, sin)
                o_s[u, 2 * j + i] = (one * c + pltpu.roll(one, HEAD // 2, 1) * s).astype(jnp.bfloat16)

        lax.fori_loop(0, (3 * heads + 1) // 2, tile, None)
        for copy in out(u):
            copy.start()

    lax.fori_loop(0, UNITS, unit, None)
    _sent(hop)

    def done(u, _):
        for copy in keep(u) + out(u):
            copy.wait()

    lax.fori_loop(0, UNITS, done, None)


def _table(rows):
    angle = np.arange(rows, dtype=np.float64)[:, None] * float(THETA) ** (-np.arange(HEAD // 2, dtype=np.float64) / (HEAD // 2))
    return jnp.asarray(np.concatenate([np.cos(angle), np.sin(angle)], -1).astype(np.float32))


def project(n, x, gain, wq, wk, wv):
    rows, d = x.shape
    heads = wq.shape[1] // HEAD
    whole = n * rows
    anywhere, vmem = pl.BlockSpec(memory_space=pl.ANY), pl.BlockSpec(memory_space=pltpu.VMEM)
    tiles = (3 * heads + 1) // 2
    split = jax.ShapeDtypeStruct((heads, whole, HEAD), jnp.bfloat16)
    return pl.pallas_call(
        functools.partial(_project, n, heads),
        out_shape=[jax.ShapeDtypeStruct((whole, d), jnp.bfloat16), split, split, split],
        in_specs=[vmem, vmem, vmem, anywhere, anywhere, anywhere],
        out_specs=[anywhere] * 4,
        scratch_shapes=[pltpu.VMEM((whole, d), jnp.bfloat16), pltpu.VMEM((d, tiles * 2 * HEAD), jnp.bfloat16),
                        pltpu.VMEM((UNITS, 2 * tiles, rows, HEAD), jnp.bfloat16), pltpu.SemaphoreType.DMA((16,)),
                        pltpu.SemaphoreType.DMA((16,)), pltpu.SemaphoreType.DMA((3,)), pltpu.SemaphoreType.DMA((UNITS, 2)),
                        pltpu.SemaphoreType.DMA((UNITS, 2, 3))],
        compiler_params=pltpu.CompilerParams(collective_id=0, has_side_effects=True, vmem_limit_bytes=MOST),
        cost_estimate=pl.CostEstimate(flops=2 * whole * d * 3 * wq.shape[1], transcendentals=0, bytes_accessed=4 * whole * d),
        name="project",
    )(x, gain[None], _table(whole), wq, wk, wv)


def _attend_gather(n, heads, dy_ref, q_ref, k_ref, v_ref, wo_ref, all_ref, do_ref, lse_ref, delta_ref, dwo_ref, buf, q_s, k_s, v_s, wo_s,
                   turned_s, sum_s, lse_s, delta_s, top_s, mix_s, gap_s, stage, send, recv, in_sem, all_sem, o_sem, end_sem,
                   stage_sem, own_sem, *, bq):
    rows, d = dy_ref.shape
    half, whole = rows // 2, n * rows
    me, peers = _peers(n)
    ready = _greet(peers)
    own = pltpu.make_async_copy(dy_ref, buf.at[pl.ds(0, rows)], own_sem)
    own.start()
    loads = [pltpu.make_async_copy(a, b, in_sem.at[i]) for i, (a, b) in enumerate(((q_ref, q_s), (k_ref, k_s), (v_ref, v_s), (wo_ref, wo_s)))]
    for load in loads:
        load.start()
    own.wait()
    ready()
    hop = functools.partial(_hop, buf, send, recv, peers, half)
    for h in FIRST:
        hop(*h).start()
    gap_s[...] = _gap(bq)
    for load in loads:
        load.wait()

    scale = HEAD**-0.5
    e = scale * LOG2E
    ones = jnp.ones((8, bq), jnp.bfloat16)

    def queries(iq, _):
        mine = pl.ds(pl.multiple_of(iq * bq, bq), bq)
        top_s[...] = jnp.full(top_s.shape, NEG, jnp.float32)
        mix_s[...] = jnp.zeros(mix_s.shape, jnp.float32)

        def block(j, masked):
            here = pl.ds(pl.multiple_of(j * bq, bq), bq)
            scores = [_dot(k_s[h, here, :], q_s[h, mine, :], 1, 1) for h in range(heads)]
            weights, keeps = [], []
            for h, s in enumerate(scores):
                if masked:
                    s = jnp.where(gap_s[...] >= 0, s, HIDDEN)
                old = top_s[h : h + 1, :]
                top = jnp.maximum(old, s.max(axis=0, keepdims=True))
                top_s[h : h + 1, :] = top
                weights.append(jnp.exp2((s - top) * e).astype(jnp.bfloat16))
                keeps.append(jnp.exp2((old - top) * e))
            for h in range(heads):
                values = jnp.concatenate([v_s[h, here, :].T, ones], axis=0)
                mix_s[h] = mix_s[h] * keeps[h] + _dot(values, weights[h], 1, 0)

        lax.fori_loop(0, iq, lambda j, _: block(j, False), None)
        block(iq, True)
        for h in range(heads):
            top, total = top_s[h : h + 1, :], mix_s[h, HEAD : HEAD + 1, :]
            o = (mix_s[h, :HEAD, :] * (1 / total)).astype(jnp.bfloat16)
            turned_s[h * HEAD : (h + 1) * HEAD, mine] = o
            q_s[h, mine, :] = o.T
            lse_s[h, :, mine] = top * scale + jnp.log(total)

    lax.fori_loop(0, whole // bq, queries, None)

    def keep(u):
        return [pltpu.make_async_copy(buf.at[pl.ds(u * rows + i * half, half)], all_ref.at[pl.ds(at, half)], all_sem.at[u, i])
                for i, at in enumerate(_rows_of(u, me, n, half))]

    def out(u):
        return [pltpu.make_async_copy(k_s.at[:, pl.ds(u * rows + i * half, half)], do_ref.at[:, pl.ds(at, half)], o_sem.at[u, i])
                for i, at in enumerate(_rows_of(u, me, n, half))]

    def unit(u, _):
        _arrive(u, hop)
        for copy in keep(u):
            copy.start()
        at = _rows_of(u, me, n, half)
        t = _dot(buf[pl.ds(pl.multiple_of(u * rows, rows), rows), :], wo_s[...], 1, 1).astype(jnp.bfloat16)
        for h in range(heads):
            one = t[:, h * HEAD : (h + 1) * HEAD]
            k_s[h, pl.ds(pl.multiple_of(u * rows, rows), rows), :] = one
            for i in range(2):
                part = one[i * half : (i + 1) * half, :].astype(jnp.float32) * q_s[h, pl.ds(at[i], half), :].astype(jnp.float32)
                delta_s[h, :, pl.ds(at[i], half)] = part.T.sum(axis=0, keepdims=True)
        for copy in out(u):
            copy.start()

    def order(u, _):
        for i, at in enumerate(_rows_of(u, me, n, half)):
            sum_s[:, pl.ds(pl.multiple_of(u * rows + i * half, half), half)] = turned_s[:, pl.ds(at, half)]

    tiles = stage.shape[0]
    w = d // tiles
    early = (UNITS - 2) * rows

    def first(j, _):
        acc_s = stage.at[j]
        acc_s[...] = jnp.dot(sum_s[:, :early], buf[:early, pl.ds(pl.multiple_of(j * w, w), w)], preferred_element_type=jnp.float32)

    lax.fori_loop(0, UNITS, order, None)
    lax.fori_loop(0, UNITS - 2, unit, None)
    lax.fori_loop(0, tiles, first, None)
    lax.fori_loop(UNITS - 2, UNITS, unit, None)

    def put(j):
        return pltpu.make_async_copy(wo_s.at[:, pl.ds(pl.multiple_of(j * w, w), w)], dwo_ref.at[:, pl.ds(pl.multiple_of(j * w, w), w)],
                                     stage_sem.at[j])

    def last(j, _):
        cols = pl.ds(pl.multiple_of(j * w, w), w)
        wo_s[:, cols] = (stage[j] + jnp.dot(sum_s[:, early:], buf[early:, cols], preferred_element_type=jnp.float32)).astype(jnp.bfloat16)
        put(j).start()

    lax.fori_loop(0, tiles, last, None)
    ends = [pltpu.make_async_copy(lse_s, lse_ref, end_sem.at[0]), pltpu.make_async_copy(delta_s, delta_ref, end_sem.at[1])]
    for copy in ends:
        copy.start()
    _sent(hop)

    def done(u, _):
        for copy in keep(u) + out(u):
            copy.wait()

    lax.fori_loop(0, UNITS, done, None)
    lax.fori_loop(0, tiles, lambda j, _: put(j).wait(), None)
    for copy in ends:
        copy.wait()


def attend_gather(n, dy, q, k, v, wo):
    rows, d = dy.shape
    heads, whole, _ = q.shape
    bq = min(512, whole)
    tiles = 20
    anywhere = pl.BlockSpec(memory_space=pl.ANY)
    bf, f32 = jnp.bfloat16, jnp.float32
    stat = jax.ShapeDtypeStruct((heads, 1, whole), f32)
    split = (heads, whole, HEAD)
    return pl.pallas_call(
        functools.partial(_attend_gather, n, heads, bq=bq),
        out_shape=[jax.ShapeDtypeStruct((whole, d), bf), jax.ShapeDtypeStruct(split, bf), stat, stat, jax.ShapeDtypeStruct(wo.shape, bf)],
        in_specs=[anywhere] * 5,
        out_specs=[anywhere] * 5,
        scratch_shapes=[pltpu.VMEM((whole, d), bf), pltpu.VMEM(split, bf), pltpu.VMEM(split, bf), pltpu.VMEM(split, bf),
                        pltpu.VMEM(wo.shape, bf), pltpu.VMEM((heads * HEAD, whole), bf),
                        pltpu.VMEM((heads * HEAD, whole), bf), pltpu.VMEM((heads, 1, whole), f32),
                        pltpu.VMEM((heads, 1, whole), f32), pltpu.VMEM((heads, bq), f32), pltpu.VMEM((heads, HEAD + 8, bq), f32),
                        pltpu.VMEM((bq, bq), jnp.int32), pltpu.VMEM((tiles, heads * HEAD, d // tiles), f32),
                        pltpu.SemaphoreType.DMA((16,)), pltpu.SemaphoreType.DMA((16,)), pltpu.SemaphoreType.DMA((4,)),
                        pltpu.SemaphoreType.DMA((UNITS, 2)), pltpu.SemaphoreType.DMA((UNITS, 2)), pltpu.SemaphoreType.DMA((2,)),
                        pltpu.SemaphoreType.DMA((tiles,)), pltpu.SemaphoreType.DMA(())],
        compiler_params=pltpu.CompilerParams(collective_id=1, has_side_effects=True, vmem_limit_bytes=MOST),
        cost_estimate=pl.CostEstimate(flops=4 * whole * d * heads * HEAD + 4 * heads * whole * whole * HEAD, transcendentals=heads * whole * whole,
                                      bytes_accessed=4 * whole * d),
        name="attend_gather",
    )(dy, q, k, v, wo)


TILES = 10


def _finish(n, heads, x_ref, dy_ref, gain_ref, dq_ref, dk_ref, dv_ref, wq_ref, wk_ref, wv_ref, some_ref, dx_ref, dgain_ref, dwq_ref, dwk_ref,
            dwv_ref, g_s, w_s, pair_s, held_s, near_s, far_s, half_s, own_s, norm_s, gains_s, g_sem, w_sem, pair_send, pair_recv, near_send,
            near_recv, far_send, far_recv, gain_send, gain_recv, a_sem, o_sem, x_sem, out_sem):
    rows, d = x_ref.shape
    wide, half, cols = heads * HEAD, rows // 2, d // TILES
    me, peers = _peers(n)
    right, left, partner = peers["right"], peers["left"], peers["partner"]
    opposite = lax.rem(me + n // 2, n)
    aside = partner - me
    slots = (opposite + aside, right + aside, opposite, left + aside, right, partner, left, me)
    f32, bf = jnp.float32, jnp.bfloat16
    barrier = pltpu.get_barrier_semaphore()
    others = [lax.rem(me + r, n) for r in range(1, n)]
    for who in others:
        pl.semaphore_signal(barrier, inc=1, device_id={"tp": who}, device_id_type=MESH)

    def rows_at(slot):
        return pl.ds(pl.multiple_of(slots[slot] * rows, rows), rows)

    loads = [[pltpu.make_async_copy(ref.at[rows_at(i)], g_s.at[pl.ds(i * rows, rows), pl.ds(m * wide, wide)], g_sem.at[i, m])
              for m, ref in enumerate((dq_ref, dk_ref, dv_ref))] for i in range(n)]

    def weights(j):
        at = pl.ds(pl.multiple_of(j * cols, cols), cols)
        return [pltpu.make_async_copy(ref.at[at], w_s.at[at, pl.ds(m * wide, wide)], w_sem.at[j, m])
                for m, ref in enumerate((wq_ref, wk_ref, wv_ref))]

    def begin(j, _):
        for copy in weights(j):
            copy.start()

    for copy in loads[0] + loads[1]:
        copy.start()
    lax.fori_loop(0, TILES, begin, None)
    for copy in sum(loads[2:], []):
        copy.start()
    pl.semaphore_wait(barrier, n - 1)

    def remote(src, dst, send, recv, who):
        return pltpu.make_async_remote_copy(src_ref=src, dst_ref=dst, send_sem=send, recv_sem=recv, device_id={"tp": who}, device_id_type=MESH)

    def pair(i, j):
        return remote(pair_s.at[i % 2, j], held_s.at[i, j], pair_send.at[i, j], pair_recv.at[i, j], partner)

    a, b = pl.ds(0, half), pl.ds(half, half)

    def near(i, j):
        return remote(held_s.at[0, j, (a, b)[i]], near_s.at[i, j], near_send.at[i, j], near_recv.at[i, j], (right, left)[i])

    def far(i, h, j):
        return remote(held_s.at[1 + i, j, (a, b)[h]], far_s.at[i, j, (a, b)[h]], far_send.at[i, h, j], far_recv.at[i, h, j], (right, left)[i])

    def term(u, j):
        at = pl.ds(pl.multiple_of(j * cols, cols), cols)
        return _dot(g_s[2 * u * rows : 2 * (u + 1) * rows, :], w_s[at, :], 1, 1)

    def arrived(u):
        for copy in loads[2 * u] + loads[2 * u + 1]:
            copy.wait()

    arrived(0)

    def unit0(j, _):
        for copy in weights(j):
            copy.wait()
        t = term(0, j)
        for i in range(2):
            pair_s[i, j] = t[i * rows : (i + 1) * rows].astype(bf)
            pair(i, j).start()

    lax.fori_loop(0, TILES, unit0, None)
    arrived(1)

    def unit1(j, _):
        t = term(1, j)
        pair(0, j).wait_recv()
        held_s[0, j] = (t[:rows] + held_s[0, j].astype(f32)).astype(bf)
        near(0, j).start()
        near(1, j).start()
        pair(0, j).wait_send()
        pair_s[0, j] = t[rows:].astype(bf)
        pair(2, j).start()

    lax.fori_loop(0, TILES, unit1, None)
    arrived(2)

    def unit2(j, _):
        t = term(2, j)
        pair(1, j).wait_recv()
        s = t[:rows] + held_s[1, j].astype(f32)
        held_s[1, j, b] = s[half:].astype(bf)
        half_s[0, j] = s[:half]
        far(0, 1, j).start()
        pair(1, j).wait_send()
        pair_s[1, j] = t[rows:].astype(bf)
        pair(3, j).start()

    lax.fori_loop(0, TILES, unit2, None)
    arrived(3)

    def unit3(j, _):
        t = term(3, j)
        pair(2, j).wait_recv()
        s = t[:rows] + held_s[2, j].astype(f32)
        held_s[2, j, a] = s[:half].astype(bf)
        half_s[1, j] = s[half:]
        far(1, 0, j).start()
        pair(3, j).wait_recv()
        own_s[j] = t[rows:] + held_s[3, j].astype(f32)

    lax.fori_loop(0, TILES, unit3, None)

    def block(m):
        return [pltpu.make_async_copy(some_ref.at[rows_at(i), pl.ds(pl.multiple_of(m * cols, cols), cols)],
                                      w_s.at[pl.ds(pl.multiple_of((m % 2) * n * rows + i * rows, rows), rows), pl.ds(0, cols)], a_sem.at[m % 2, i])
                for i in range(n)]

    def put(m):
        base = 2 * n * rows
        return [pltpu.make_async_copy(w_s.at[pl.ds(pl.multiple_of(base + (m % 2) * cols, cols), cols), pl.ds(i * wide, wide)],
                                      ref.at[pl.ds(pl.multiple_of(m * cols, cols), cols)], o_sem.at[m % 2, i])
                for i, ref in enumerate((dwq_ref, dwk_ref, dwv_ref))]

    def middle(j, _):
        for i in range(2):
            near(i, j).wait_recv()
            held_s[1 + i, j, (a, b)[i]] = (half_s[i, j] + near_s[i, j].astype(f32)).astype(bf)
            far(i, i, j).start()
            near(i, j).wait_send()
        for i in range(2):
            pair(2 + i, j).wait_send()
        for copy in inputs(j):
            copy.start()

    def inputs(j):
        return [pltpu.make_async_copy(ref.at[:, pl.ds(pl.multiple_of(j * cols, cols), cols)], pair_s.at[i, j], x_sem.at[i, j])
                for i, ref in enumerate((x_ref, dy_ref))]

    for copy in block(0):
        copy.start()

    def weight(m, _):
        @pl.when(m + 1 < TILES)
        def _():
            for copy in block(m + 1):
                copy.start()

        @pl.when(m == 2)
        def _():
            lax.fori_loop(0, TILES, middle, None)

        @pl.when(m >= 2)
        def _():
            for copy in put(m - 2):
                copy.wait()

        for copy in block(m):
            copy.wait()
        t = w_s[pl.ds(pl.multiple_of((m % 2) * n * rows, rows), n * rows), :cols]
        to = pl.ds(pl.multiple_of(2 * n * rows + (m % 2) * cols, cols), cols)
        for i in range(3):
            w_s[to, i * wide : (i + 1) * wide] = _dot(t, g_s[:, i * wide : (i + 1) * wide], 0, 0).astype(bf)
        for copy in put(m):
            copy.start()

    lax.fori_loop(0, TILES, weight, None)

    def last(j, _):
        for i in range(2):
            for h in range(2):
                far(i, h, j).wait_recv()
        for copy in inputs(j):
            copy.wait()

    lax.fori_loop(0, TILES, last, None)
    norm_s[...] = jnp.zeros_like(norm_s)

    def derive(r, _):
        at = pl.ds(pl.multiple_of(r * 16, 16), 16)

        def d_some(j):
            return own_s[j, at, :] + far_s[0, j, at, :].astype(f32) + far_s[1, j, at, :].astype(f32)

        xs = [pair_s[0, j, at, :].astype(f32) for j in range(TILES)]
        scale = lax.rsqrt(sum((t * t).sum(-1, keepdims=True) for t in xs) * (1 / d) + 1e-6)
        mean = jnp.zeros((16, 1), f32)
        for j in range(TILES):
            g = d_some(j) * (xs[j] * scale)
            norm_s[j] += g
            mean += (g * gain_ref[:, j * cols : (j + 1) * cols].astype(f32)).sum(-1, keepdims=True)
        mean = mean * (1 / d)
        for j in range(TILES):
            by_x = scale * (d_some(j) * gain_ref[:, j * cols : (j + 1) * cols].astype(f32) - xs[j] * scale * mean)
            pair_s[1, j, at, :] = (pair_s[1, j, at, :].astype(f32) + by_x.astype(bf).astype(f32)).astype(bf)

    lax.fori_loop(0, rows // 16, derive, None)
    for j in range(TILES):
        gains_s[0, :, j * cols : (j + 1) * cols] = norm_s[j].sum(axis=0, keepdims=True)

    def results(j):
        return pltpu.make_async_copy(pair_s.at[1, j], dx_ref.at[:, pl.ds(pl.multiple_of(j * cols, cols), cols)], out_sem.at[j])

    lax.fori_loop(0, TILES, lambda j, _: results(j).start(), None)
    gains = [remote(gains_s.at[0], gains_s.at[1 + r], gain_send.at[r], gain_recv.at[r], who) for r, who in enumerate(others)]
    for copy in gains:
        copy.start()

    def close(j, _):
        for i in range(2):
            for h in range(2):
                far(i, h, j).wait_send()
        results(j).wait()

    lax.fori_loop(0, TILES, close, None)
    for m in range(TILES - 2, TILES):
        for copy in put(m):
            copy.wait()
    for copy in gains:
        copy.wait()
    total = jnp.zeros((1, d), f32)
    for r in range(n):
        total += gains_s[lax.rem(me + n - r, n)]
    dgain_ref[...] = total


def finish(n, x, dy, gain, dq, dk, dv, wq, wk, wv, some):
    rows, d = x.shape
    heads = wq.shape[1] // HEAD
    cols, half, wide = d // TILES, rows // 2, wq.shape[1]
    f32, bf = jnp.float32, jnp.bfloat16
    anywhere, vmem = pl.BlockSpec(memory_space=pl.ANY), pl.BlockSpec(memory_space=pltpu.VMEM)
    sem = pltpu.SemaphoreType.DMA
    weight = jax.ShapeDtypeStruct(wq.shape, bf)
    return pl.pallas_call(
        functools.partial(_finish, n, heads),
        out_shape=[jax.ShapeDtypeStruct(x.shape, bf), jax.ShapeDtypeStruct((1, d), f32), weight, weight, weight],
        in_specs=[anywhere, anywhere, vmem] + [anywhere] * 7,
        out_specs=[anywhere, vmem] + [anywhere] * 3,
        scratch_shapes=[pltpu.VMEM((n * rows, 3 * wide), bf), pltpu.VMEM((d, 3 * wide), bf), pltpu.VMEM((2, TILES, rows, cols), bf),
                        pltpu.VMEM((4, TILES, rows, cols), bf), pltpu.VMEM((2, TILES, half, cols), bf), pltpu.VMEM((2, TILES, rows, cols), bf),
                        pltpu.VMEM((2, TILES, half, cols), f32), pltpu.VMEM((TILES, rows, cols), f32), pltpu.VMEM((TILES, 16, cols), f32),
                        pltpu.VMEM((n, 1, d), f32), sem((n, 3)), sem((TILES, 3)), sem((4, TILES)), sem((4, TILES)), sem((2, TILES)),
                        sem((2, TILES)), sem((2, 2, TILES)), sem((2, 2, TILES)), sem((n - 1,)), sem((n - 1,)), sem((2, n)), sem((2, 3)),
                        sem((2, TILES)), sem((TILES,))],
        compiler_params=pltpu.CompilerParams(collective_id=2, has_side_effects=True, vmem_limit_bytes=MOST),
        cost_estimate=pl.CostEstimate(flops=12 * n * rows * d * wide, transcendentals=0, bytes_accessed=6 * n * rows * d),
        name="finish",
    )(x, dy, gain[None], dq, dk, dv, wq, wk, wv, some)


def solution(mesh):
    n = mesh.shape["tp"]

    def step(x, dy, gain, wq, wk, wv, wo):
        some, q, k, v = project(n, x, gain, wq, wk, wv)
        _, d_seen, lse, delta, dwo = attend_gather(n, dy, q, k, v, wo)
        dq, dk, dv = attend_bwd(q, k, v, d_seen, lse, delta, min(512, q.shape[1]))
        dx, dgain, dwq, dwk, dwv = finish(n, x, dy, gain, dq, dk, dv, wq, wk, wv, some)
        return dx, dgain, dwq, dwk, dwv, dwo

    tokens, columns = P(("dp", "tp"), None), P(None, "tp")
    return jax.shard_map(
        step,
        mesh=mesh,
        in_specs=(tokens, tokens, P(None), columns, columns, columns, P("tp", None)),
        out_specs=(tokens, P("dp", None), P("dp", "tp"), P("dp", "tp"), P("dp", "tp"), P(("dp", "tp"), None)),
        check_vma=False,
    )
```

```python
import functools

import jax
import jax.numpy as jnp
import numpy as np
from jax import lax
from jax.experimental import pallas as pl
from jax.experimental.pallas import tpu as pltpu
from jax.sharding import PartitionSpec as P

NEG = -1e30
HIDDEN = 2 * NEG
LOG2E = 1.4426950408889634
HEAD = 128
THETA = 10000
MOST = 64 * 2**20 - 64 * 1024
MESH = pl.DeviceIdType.MESH
DMA = pltpu.SemaphoreType.DMA


def _dot(a, b, ca, cb):
    return lax.dot_general(a, b, (((ca,), (cb,)), ((), ())), preferred_element_type=jnp.float32)


def _loop(count, body, first=0):
    lax.fori_loop(first, count, body, None)


def _gap(bq):
    return lax.broadcasted_iota(jnp.int32, (bq, bq), 1) - lax.broadcasted_iota(jnp.int32, (bq, bq), 0)


def _spread(turn):
    left = lax.broadcasted_iota(jnp.int32, turn.shape, 1) < HEAD // 2
    other = pltpu.roll(turn, HEAD // 2, 1)
    return jnp.where(left, turn, other), jnp.where(left, -other, turn)


def _backward(q_ref, k_ref, v_ref, do_ref, lse_ref, delta_ref, turn_ref, dwo_ref, dq_ref, dk_ref, dv_ref, out_ref, dq_s, dk_s, dv_s, gap_s):
    out_ref[...] = dwo_ref[...]
    heads, bq, _ = q_ref.shape
    iq = pl.program_id(0)
    scale = HEAD**-0.5
    e = scale * LOG2E

    @pl.when(iq == 0)
    def _():
        gap_s[...] = _gap(bq)
        dk_s[...] = jnp.zeros_like(dk_s)
        dv_s[...] = jnp.zeros_like(dv_s)

    dq_s[...] = jnp.zeros_like(dq_s)
    lses = [lse_ref[h] * LOG2E for h in range(heads)]
    deltas = [delta_ref[h] for h in range(heads)]

    def block(first, size, ahead, masked):
        here, mine = pl.ds(pl.multiple_of(first, size), size), slice(ahead, bq)
        scores = [_dot(k_ref[h, here, :], q_ref[h, mine, :], 1, 1) for h in range(heads)]
        dps = [_dot(v_ref[h, here, :], do_ref[h, mine, :], 1, 1) for h in range(heads)]
        for h in range(heads):
            p = jnp.exp2(scores[h] * e - lses[h][:, mine])
            if masked:
                p = jnp.where(gap_s[:size, : bq - ahead] >= 0, p, 0.0)
            ds = (p * (dps[h] - deltas[h][:, mine])).astype(jnp.bfloat16)
            dv_s[h, here, :] += _dot(p.astype(jnp.bfloat16), do_ref[h, mine, :], 1, 0)
            dk_s[h, here, :] += _dot(ds, q_ref[h, mine, :], 1, 0)
            dq_s[h, :, mine] += _dot(k_ref[h, here, :].T, ds, 1, 0)

    _loop(iq, lambda j, _: block(j * bq, bq, 0, False))
    half = bq // 2
    block(iq * bq, half, 0, True)
    block(iq * bq + half, half, half, True)

    def back(g, cos, sin):
        g = g.astype(jnp.bfloat16).astype(jnp.float32)
        return (g * cos - pltpu.roll(g, HEAD // 2, 1) * sin).astype(jnp.bfloat16)

    cos, sin = _spread(turn_ref[pl.ds(pl.multiple_of(iq * bq, bq), bq), :])
    for h in range(heads):
        dq_ref[:, h * HEAD : (h + 1) * HEAD] = back((dq_s[h] * scale).T, cos, sin)

    @pl.when(iq == pl.num_programs(0) - 1)
    def _():
        def rows(r, _):
            at = pl.ds(pl.multiple_of(r * bq, bq), bq)
            cos, sin = _spread(turn_ref[at, :])
            for h in range(heads):
                lanes = slice(h * HEAD, (h + 1) * HEAD)
                dk_ref[at, lanes] = back(dk_s[h, at, :] * scale, cos, sin)
                dv_ref[at, lanes] = dv_s[h, at, :].astype(jnp.bfloat16)

        _loop(pl.num_programs(0), rows)


def attend_bwd(q, k, v, d_out, lse, delta, dwo, bq):
    heads, whole, _ = q.shape
    blocks = pl.BlockSpec((heads, bq, HEAD), lambda i: (0, i, 0))
    full = pl.BlockSpec((heads, whole, HEAD), lambda i: (0, 0, 0))
    stat = pl.BlockSpec((heads, 1, bq), lambda i: (0, 0, i))
    flat = jax.ShapeDtypeStruct((whole, heads * HEAD), jnp.bfloat16)
    all_rows = pl.BlockSpec(flat.shape, lambda i: (0, 0))
    some_rows = pl.BlockSpec((dwo.shape[0] * bq // whole, dwo.shape[1]), lambda i: (i, 0))
    return pl.pallas_call(
        _backward,
        grid=(whole // bq,),
        in_specs=[blocks, full, full, blocks, stat, stat, pl.BlockSpec((whole, HEAD), lambda i: (0, 0)), some_rows],
        out_specs=[pl.BlockSpec((bq, heads * HEAD), lambda i: (i, 0)), all_rows, all_rows, some_rows],
        out_shape=[flat] * 3 + [jax.ShapeDtypeStruct(dwo.shape, dwo.dtype)],
        scratch_shapes=[pltpu.VMEM((heads, HEAD, bq), jnp.float32), pltpu.VMEM((heads, whole, HEAD), jnp.float32),
                        pltpu.VMEM((heads, whole, HEAD), jnp.float32), pltpu.VMEM((bq, bq), jnp.int32)],
        compiler_params=pltpu.CompilerParams(dimension_semantics=("arbitrary",), vmem_limit_bytes=MOST),
        cost_estimate=pl.CostEstimate(flops=5 * heads * whole * whole * HEAD, transcendentals=heads * whole * whole, bytes_accessed=14 * q.size),
        name="attend_bwd",
    )(q, k, v, d_out, lse, delta, _table(whole), dwo)


EARLY = ((0, 4, "right"), (1, 5, "left"), (0, 2, "partner"), (1, 3, "partner"))
REST = ((1, 8, "right"), (0, 9, "left"))
ON = ((4, 12, "right"), (5, 13, "left"), (4, 6, "partner"), (5, 7, "partner"))
LATE = {4: ((8, 10, "partner"), (9, 11, "partner")), 6: ((12, 14, "partner"), (13, 15, "partner"))}
WHOLE = (EARLY + REST, {2: ON, **LATE})
REMAINDER = (REST + ON, LATE)
UNITS = 8
TILES = 10


def _peers(n):
    me = lax.axis_index("tp")
    partner = me + 1 - 2 * lax.rem(me, 2)
    return me, {"right": lax.rem(me + 2, n), "left": lax.rem(me + n - 2, n), "partner": partner}


def _greet(peers):
    barrier = pltpu.get_barrier_semaphore()
    for who in peers.values():
        pl.semaphore_signal(barrier, inc=1, device_id={"tp": who}, device_id_type=MESH)
    return lambda: pl.semaphore_wait(barrier, len(peers))


def _rows_of(u, me, n, half):
    s = u // 2
    base = me + (u % 2) * (1 - 2 * (me % 2))
    mid, far = (s * (3 - s)) // 2, s // 3
    a = (base + n - 2 * mid + (n // 2) * far) % n
    b = (base + 2 * mid + (n // 2) * far) % n
    h = s // 2 - far
    return pl.multiple_of((2 * a + h) * half, half), pl.multiple_of((2 * b + 1 - h) * half, half)


def _hop(buf, send, recv, peers, half, src, dst, whom):
    return pltpu.make_async_remote_copy(src_ref=buf.at[pl.ds(src * half, half)], dst_ref=buf.at[pl.ds(dst * half, half)],
                                        send_sem=send.at[dst], recv_sem=recv.at[dst], device_id={"tp": peers[whom]}, device_id_type=MESH)


def _arrive(u, hop, plan, at=None):
    first, then = plan
    for k in range(1, UNITS):
        @pl.when(u == k)
        def _():
            for src, dst, whom in sum(then.values(), first):
                if dst // 2 == k:
                    hop(src, dst, whom).wait_recv()
            for h in then.get(k, ()):
                hop(*h).start()
            for copy in (at or {}).get(k, ()):
                copy.start()


def _sent(hop, plan):
    first, then = plan
    for h in sum(then.values(), first):
        hop(*h).wait_send()


def _project(n, heads, x_ref, gain_ref, turn_ref, dy_ref, wq_ref, wk_ref, wv_ref, wo_ref, all_ref, q_ref, k_ref, v_ref, early_ref, wt_ref, wot_ref,
             buf, w_s, o_s, all_s, wt_s, wo_s, wot_s, send, recv, early_send, early_recv, w_sem, all_sem, o_sem, wt_sem, wo_sem, wot_sem):
    rows, d = x_ref.shape
    half, wide = rows // 2, heads * HEAD
    me, peers = _peers(n)
    ready = _greet(peers)
    loads = [pltpu.make_async_copy(w, w_s.at[:, pl.ds(i * wide, wide)], w_sem.at[i]) for i, w in enumerate((wq_ref, wk_ref, wv_ref))]
    for load in loads:
        load.start()
    gain = gain_ref[...].astype(jnp.float32)

    def norm(i, _):
        at = pl.ds(pl.multiple_of(i * 16, 16), 16)
        t = x_ref[at, :].astype(jnp.float32)
        scale = lax.rsqrt(jnp.mean(t * t, -1, keepdims=True) + 1e-6)
        buf[at, :] = (t * scale * gain).astype(jnp.bfloat16)

    _loop(rows // 16, norm)
    ready()
    hop = functools.partial(_hop, buf, send, recv, peers, half)
    for h in WHOLE[0]:
        hop(*h).start()
    early = [pltpu.make_async_remote_copy(src_ref=dy_ref.at[pl.ds(src * half, half)], dst_ref=early_ref.at[pl.ds((dst - 2) * half, half)],
                                          send_sem=early_send.at[dst - 2], recv_sem=early_recv.at[dst - 2], device_id={"tp": peers[whom]},
                                          device_id_type=MESH) for src, dst, whom in EARLY]
    for load in loads:
        load.wait()

    def keep(u):
        return [pltpu.make_async_copy(all_s.at[:, pl.ds(i * half, half)], all_ref.at[:, pl.ds(at, half)], all_sem.at[i])
                for i, at in enumerate(_rows_of(u, me, n, half))]

    cols = d // TILES

    def weights_out(j):
        i = j % 2
        return [pltpu.make_async_copy(wt_s.at[i], wt_ref.at[j], wt_sem.at[i]),
                pltpu.make_async_copy(wot_s.at[i], wot_ref.at[pl.ds(pl.multiple_of(j * cols, cols), cols)], wot_sem.at[i])]

    def wo_in(j):
        return pltpu.make_async_copy(wo_ref.at[:, pl.ds(pl.multiple_of(j * cols, cols), cols)], wo_s.at[j % 2], wo_sem.at[j % 2])

    def flip(j):
        i = j % 2

        @pl.when(j >= 2)
        def _():
            for copy in weights_out(j - 2):
                copy.wait()

        wo_in(j).wait()
        wt_s[i] = w_s[pl.ds(pl.multiple_of(j * cols, cols), cols), : 3 * wide].T
        wot_s[i] = wo_s[i].T
        for copy in weights_out(j):
            copy.start()

        @pl.when(j + 2 < TILES)
        def _():
            wo_in(j + 2).start()

    for j in range(2):
        wo_in(j).start()

    def out(u):
        return [pltpu.make_async_copy(o_s.at[u, pl.ds(m * heads, heads), pl.ds(i * half, half)], ref.at[:, pl.ds(at, half)],
                                      o_sem.at[u, i, m])
                for i, at in enumerate(_rows_of(u, me, n, half)) for m, ref in enumerate((q_ref, k_ref, v_ref))]

    def unit(u, _):
        _arrive(u, hop, WHOLE, {4: early})
        a, b = _rows_of(u, me, n, half)
        cos, sin = _spread(jnp.concatenate([turn_ref[pl.ds(a, half), :], turn_ref[pl.ds(b, half), :]], axis=0))

        def tile(j, _):
            t = jnp.dot(buf[pl.ds(pl.multiple_of(u * rows, rows), rows), :], w_s[:, pl.ds(pl.multiple_of(j * 2 * HEAD, 2 * HEAD), 2 * HEAD)],
                        preferred_element_type=jnp.float32).astype(jnp.bfloat16)
            for i in range(2):
                one = t[:, i * HEAD : (i + 1) * HEAD].astype(jnp.float32)
                straight = 2 * j + i >= 2 * heads
                c, s = jnp.where(straight, 1.0, cos), jnp.where(straight, 0.0, sin)
                o_s[u, 2 * j + i] = (one * c + pltpu.roll(one, HEAD // 2, 1) * s).astype(jnp.bfloat16)

        _loop((3 * heads + 1) // 2, tile)
        for copy in out(u):
            copy.start()

        @pl.when(u >= 1)
        def _():
            for copy in keep(u - 1):
                copy.wait()

        def column(c, _):
            at = pl.ds(pl.multiple_of(c * cols, cols), cols)
            all_s[at, :] = buf[pl.ds(pl.multiple_of(u * rows, rows), rows), at].T

        _loop(TILES, column)
        for copy in keep(u):
            copy.start()

        @pl.when(u < TILES // 2)
        def _():
            _loop(2 * u + 2, lambda j, _: flip(j), 2 * u)

    _loop(UNITS, unit)
    _sent(hop, WHOLE)
    for copy in early:
        copy.wait()

    def done(u, _):
        for copy in out(u):
            copy.wait()

    _loop(UNITS, done)
    for copy in keep(UNITS - 1) + weights_out(TILES - 2) + weights_out(TILES - 1):
        copy.wait()


def _table(rows):
    angle = np.arange(rows, dtype=np.float64)[:, None] * float(THETA) ** (-np.arange(HEAD // 2, dtype=np.float64) / (HEAD // 2))
    return jnp.asarray(np.concatenate([np.cos(angle), np.sin(angle)], -1).astype(np.float32))


def project(n, x, dy, gain, wq, wk, wv, wo):
    rows, d = x.shape
    heads = wq.shape[1] // HEAD
    whole, wide, cols, bf = n * rows, wq.shape[1], d // TILES, jnp.bfloat16
    anywhere, vmem = pl.BlockSpec(memory_space=pl.ANY), pl.BlockSpec(memory_space=pltpu.VMEM)
    tiles = (3 * heads + 1) // 2
    split = jax.ShapeDtypeStruct((heads, whole, HEAD), jnp.bfloat16)
    return pl.pallas_call(
        functools.partial(_project, n, heads),
        out_shape=[jax.ShapeDtypeStruct((d, whole), bf), split, split, split, jax.ShapeDtypeStruct((2 * rows, d), bf),
                   jax.ShapeDtypeStruct((TILES, 3 * wide, cols), bf), jax.ShapeDtypeStruct((d, wide), bf)],
        in_specs=[vmem, vmem, vmem] + [anywhere] * 5,
        out_specs=[anywhere] * 7,
        scratch_shapes=[pltpu.VMEM((whole, d), jnp.bfloat16), pltpu.VMEM((d, tiles * 2 * HEAD), jnp.bfloat16),
                        pltpu.VMEM((UNITS, 2 * tiles, rows, HEAD), bf), pltpu.VMEM((d, rows), bf), pltpu.VMEM((2, 3 * wide, cols), bf),
                        pltpu.VMEM((2, wide, cols), bf), pltpu.VMEM((2, cols, wide), bf), DMA((16,)),
                        DMA((16,)), DMA((4,)), DMA((4,)),
                        DMA((3,)), DMA((2,)), DMA((UNITS, 2, 3)),
                        DMA((2,)), DMA((2,)), DMA((2,))],
        compiler_params=pltpu.CompilerParams(collective_id=0, has_side_effects=True, vmem_limit_bytes=MOST),
        cost_estimate=pl.CostEstimate(flops=2 * whole * d * 3 * wq.shape[1], transcendentals=0, bytes_accessed=4 * whole * d),
        name="project",
    )(x, gain[None], _table(whole), dy, wq, wk, wv, wo)


def _attend_gather(n, heads, dy_ref, early_ref, q_ref, k_ref, v_ref, wo_ref, do_ref, lse_ref, delta_ref, dwo_ref, buf, q_s, k_s, v_s, wo_s,
                   turned_s, sum_s, lse_s, delta_s, top_s, mix_s, gap_s, stage, dwo_s, send, recv, in_sem, o_sem, end_sem,
                   stage_sem, own_sem, *, bq):
    rows, d = dy_ref.shape
    half, whole = rows // 2, n * rows
    me, peers = _peers(n)
    ready = _greet(peers)
    own = pltpu.make_async_copy(dy_ref, buf.at[pl.ds(0, rows)], own_sem.at[0])
    own.start()
    come = pltpu.make_async_copy(early_ref, buf.at[pl.ds(rows, 2 * rows)], own_sem.at[1])
    come.start()
    loads = [pltpu.make_async_copy(a, b, in_sem.at[i]) for i, (a, b) in enumerate(((q_ref, q_s), (k_ref, k_s), (v_ref, v_s), (wo_ref, wo_s)))]
    for load in loads:
        load.start()
    own.wait()
    ready()
    hop = functools.partial(_hop, buf, send, recv, peers, half)
    for h in REST:
        hop(*h).start()
    come.wait()
    for h in ON:
        hop(*h).start()
    gap_s[...] = _gap(bq)
    for load in loads:
        load.wait()

    scale = HEAD**-0.5
    e = scale * LOG2E
    ones = jnp.ones((8, bq), jnp.bfloat16)

    def queries(iq, _):
        mine = pl.ds(pl.multiple_of(iq * bq, bq), bq)
        top_s[...] = jnp.full(top_s.shape, NEG, jnp.float32)
        mix_s[...] = jnp.zeros(mix_s.shape, jnp.float32)

        def block(j, masked):
            here = pl.ds(pl.multiple_of(j * bq, bq), bq)
            scores = [_dot(k_s[h, here, :], q_s[h, mine, :], 1, 1) for h in range(heads)]
            weights, keeps = [], []
            for h, s in enumerate(scores):
                if masked:
                    s = jnp.where(gap_s[...] >= 0, s, HIDDEN)
                old = top_s[h : h + 1, :]
                top = jnp.maximum(old, s.max(axis=0, keepdims=True))
                top_s[h : h + 1, :] = top
                weights.append(jnp.exp2((s - top) * e).astype(jnp.bfloat16))
                keeps.append(jnp.exp2((old - top) * e))
            for h in range(heads):
                values = jnp.concatenate([v_s[h, here, :].T, ones], axis=0)
                mix_s[h] = mix_s[h] * keeps[h] + _dot(values, weights[h], 1, 0)

        _loop(iq, lambda j, _: block(j, False))
        block(iq, True)
        for h in range(heads):
            top, total = top_s[h : h + 1, :], mix_s[h, HEAD : HEAD + 1, :]
            o = (mix_s[h, :HEAD, :] * (1 / total)).astype(jnp.bfloat16)
            turned_s[h * HEAD : (h + 1) * HEAD, mine] = o
            q_s[h, mine, :] = o.T
            lse_s[h, :, mine] = top * scale + jnp.log(total)

    _loop(whole // bq, queries)

    def out(u):
        return [pltpu.make_async_copy(k_s.at[:, pl.ds(u * rows + i * half, half)], do_ref.at[:, pl.ds(at, half)], o_sem.at[u, i])
                for i, at in enumerate(_rows_of(u, me, n, half))]

    def unit(u, _):
        _arrive(u, hop, REMAINDER)
        at = _rows_of(u, me, n, half)
        t = jnp.dot(buf[pl.ds(pl.multiple_of(u * rows, rows), rows), :], wo_s[...], preferred_element_type=jnp.float32).astype(jnp.bfloat16)
        for h in range(heads):
            one = t[:, h * HEAD : (h + 1) * HEAD]
            k_s[h, pl.ds(pl.multiple_of(u * rows, rows), rows), :] = one
            for i in range(2):
                part = one[i * half : (i + 1) * half, :].astype(jnp.float32) * q_s[h, pl.ds(at[i], half), :].astype(jnp.float32)
                delta_s[h, :, pl.ds(at[i], half)] = part.T.sum(axis=0, keepdims=True)
        for copy in out(u):
            copy.start()

    def order(u, _):
        for i, at in enumerate(_rows_of(u, me, n, half)):
            sum_s[:, pl.ds(pl.multiple_of(u * rows + i * half, half), half)] = turned_s[:, pl.ds(at, half)]

    tiles = stage.shape[0]
    w = d // tiles
    early = (UNITS - 2) * rows

    def first(j, _):
        acc_s = stage.at[j]
        acc_s[...] = jnp.dot(sum_s[:, :early], buf[:early, pl.ds(pl.multiple_of(j * w, w), w)], preferred_element_type=jnp.float32)

    _loop(UNITS, order)
    _loop(UNITS - 2, unit)
    _loop(tiles, first)
    _loop(UNITS, unit, UNITS - 2)

    def put(j):
        return pltpu.make_async_copy(dwo_s.at[j % 2], dwo_ref.at[:, pl.ds(pl.multiple_of(j * w, w), w)], stage_sem.at[j % 2])

    def last(j, _):
        @pl.when(j >= 2)
        def _():
            put(j - 2).wait()

        cols = pl.ds(pl.multiple_of(j * w, w), w)
        dwo_s[j % 2] = (stage[j] + jnp.dot(sum_s[:, early:], buf[early:, cols], preferred_element_type=jnp.float32)).astype(jnp.bfloat16)
        put(j).start()

    _loop(tiles, last)
    ends = [pltpu.make_async_copy(lse_s, lse_ref, end_sem.at[0]), pltpu.make_async_copy(delta_s, delta_ref, end_sem.at[1])]
    for copy in ends:
        copy.start()
    _sent(hop, REMAINDER)

    def done(u, _):
        for copy in out(u):
            copy.wait()

    _loop(UNITS, done)
    for j in range(tiles - 2, tiles):
        put(j).wait()
    for copy in ends:
        copy.wait()


def attend_gather(n, dy, early, q, k, v, wot):
    rows, d = dy.shape
    heads, whole, _ = q.shape
    bq = min(512, whole)
    tiles = 20
    anywhere = pl.BlockSpec(memory_space=pl.ANY)
    bf, f32 = jnp.bfloat16, jnp.float32
    stat = jax.ShapeDtypeStruct((heads, 1, whole), f32)
    split = (heads, whole, HEAD)
    return pl.pallas_call(
        functools.partial(_attend_gather, n, heads, bq=bq),
        out_shape=[jax.ShapeDtypeStruct(split, bf), stat, stat, jax.ShapeDtypeStruct(wot.shape[::-1], bf)],
        in_specs=[anywhere] * 6,
        out_specs=[anywhere] * 4,
        scratch_shapes=[pltpu.VMEM((whole, d), bf), pltpu.VMEM(split, bf), pltpu.VMEM(split, bf), pltpu.VMEM(split, bf),
                        pltpu.VMEM(wot.shape, bf), pltpu.VMEM((heads * HEAD, whole), bf),
                        pltpu.VMEM((heads * HEAD, whole), bf), pltpu.VMEM((heads, 1, whole), f32),
                        pltpu.VMEM((heads, 1, whole), f32), pltpu.VMEM((heads, bq), f32), pltpu.VMEM((heads, HEAD + 8, bq), f32),
                        pltpu.VMEM((bq, bq), jnp.int32), pltpu.VMEM((tiles, heads * HEAD, d // tiles), f32), pltpu.VMEM((2, heads * HEAD, d // tiles), bf),
                        DMA((16,)), DMA((16,)), DMA((4,)),
                        DMA((UNITS, 2)), DMA((2,)),
                        DMA((2,)), DMA((2,))],
        compiler_params=pltpu.CompilerParams(collective_id=1, has_side_effects=True, vmem_limit_bytes=MOST),
        cost_estimate=pl.CostEstimate(flops=4 * whole * d * heads * HEAD + 4 * heads * whole * whole * HEAD, transcendentals=heads * whole * whole,
                                      bytes_accessed=4 * whole * d),
        name="attend_gather",
    )(dy, early, q, k, v, wot)


AHEAD = 3


def _finish(n, heads, x_ref, dy_ref, gain_ref, dq_ref, dk_ref, dv_ref, wt_ref, all_ref, dx_ref, dgain_ref, dwq_ref, dwk_ref,
            g_s, w_s, pair_s, held_s, near_s, far_s, half_s, own_s, ahead_s, norm_s, scale_s, mean_s, gains_s, g_sem, w_sem, pair_send, pair_recv, near_send,
            near_recv, far_send, far_recv, gain_send, gain_recv, a_sem, o_sem, x_sem, out_sem):
    rows, d = x_ref.shape
    wide, half, cols = heads * HEAD, rows // 2, d // TILES
    me, peers = _peers(n)
    right, left, partner = peers["right"], peers["left"], peers["partner"]
    opposite = lax.rem(me + n // 2, n)
    aside = partner - me
    slots = (opposite + aside, opposite, right + aside, left + aside, right, left, partner, me)
    f32, bf = jnp.float32, jnp.bfloat16
    barrier = pltpu.get_barrier_semaphore()
    others = [lax.rem(me + r, n) for r in range(1, n)]
    for who in others:
        pl.semaphore_signal(barrier, inc=1, device_id={"tp": who}, device_id_type=MESH)

    def rows_at(slot):
        return pl.ds(pl.multiple_of(slots[slot] * rows, rows), rows)

    loads = [[pltpu.make_async_copy(ref.at[rows_at(i)], g_s.at[pl.ds(i * rows, rows), pl.ds(m * wide, wide)], g_sem.at[i, m])
              for m, ref in enumerate((dq_ref, dk_ref, dv_ref))] for i in range(n)]

    def weights(j):
        return pltpu.make_async_copy(wt_ref.at[j], w_s.at[j], w_sem.at[j])

    for copy in loads[0] + loads[1]:
        copy.start()
    _loop(TILES, lambda j, _: weights(j).start())
    for copy in sum(loads[2:], []):
        copy.start()
    pl.semaphore_wait(barrier, n - 1)

    def remote(src, dst, send, recv, who):
        return pltpu.make_async_remote_copy(src_ref=src, dst_ref=dst, send_sem=send, recv_sem=recv, device_id={"tp": who}, device_id_type=MESH)

    def pair(i, j):
        return remote(pair_s.at[i % 2, j], held_s.at[i, j], pair_send.at[i, j], pair_recv.at[i, j], partner)

    a, b = pl.ds(0, half), pl.ds(half, half)

    def near(i, j):
        return remote(held_s.at[0, j, (a, b)[i]], near_s.at[i, j], near_send.at[i, j], near_recv.at[i, j], (right, left)[i])

    def far(i, h, j):
        return remote(held_s.at[1 + i, j, (a, b)[h]], far_s.at[i, j, (a, b)[h]], far_send.at[i, h, j], far_recv.at[i, h, j], (right, left)[i])

    def term(u, j):
        return jnp.dot(g_s[2 * u * rows : 2 * (u + 1) * rows, :], w_s[j], preferred_element_type=f32)

    def arrived(u):
        for copy in loads[2 * u] + loads[2 * u + 1]:
            copy.wait()

    arrived(0)

    def both(j):
        pair(0, j).wait_recv()
        held_s[0, j] = (ahead_s[j % AHEAD] + held_s[0, j].astype(f32)).astype(bf)
        near(0, j).start()
        near(1, j).start()

    def unit0(j, _):
        weights(j).wait()
        t = term(0, j)
        pair_s[0, j] = t[:rows].astype(bf)
        pair(0, j).start()
        ahead_s[j % AHEAD] = t[rows:]

        @pl.when(j >= AHEAD - 1)
        def _():
            both(j - (AHEAD - 1))

    _loop(TILES, unit0)
    for j in range(TILES - AHEAD + 1, TILES):
        both(j)
    arrived(1)

    def unit1(j, _):
        t = term(1, j)
        pair_s[1, j] = t[:rows].astype(bf)
        pair(1, j).start()
        pair(0, j).wait_send()
        pair_s[0, j] = t[rows:].astype(bf)
        pair(2, j).start()

    _loop(TILES, unit1)
    arrived(2)

    def unit2(j, _):
        t = term(2, j)
        for i in range(2):
            pair(1 + i, j).wait_recv()
            t_i = t[i * rows : (i + 1) * rows] + held_s[1 + i, j].astype(f32)
            mine = (a, b)[1 - i]
            first, second = t_i[:half], t_i[half:]
            held_s[1 + i, j, mine] = (second, first)[i].astype(bf)
            half_s[i, j] = (first, second)[i]
            far(i, 1 - i, j).start()

    _loop(TILES, unit2)
    arrived(3)

    def unit3(j, _):
        t = term(3, j)
        pair(1, j).wait_send()
        pair_s[1, j] = t[:rows].astype(bf)
        pair(3, j).start()
        own_s[j] = t[rows:]

    _loop(TILES, unit3)

    depth, width = n * rows // cols, -(-2 * wide // cols)
    per = 3 * wide // cols

    def spot(k):
        return w_s.at[k // per, pl.ds(pl.multiple_of((k % per) * cols, cols), cols)]

    def block(m):
        return [pltpu.make_async_copy(all_ref.at[pl.ds(pl.multiple_of(m * cols, cols), cols), rows_at(i)],
                                      spot((m % 2) * depth + i * rows // cols).at[:, pl.ds(i * rows % cols, rows)], a_sem.at[m % 2, i])
                for i in range(n)]

    def made(m, c):
        return spot(2 * depth + (m % 2) * width + c)

    cuts = sorted({c * cols for c in range(width)} | {0, wide, 2 * wide})

    def put(m):
        return [pltpu.make_async_copy(made(m, p // cols).at[:, pl.ds(p % cols, q - p)],
                                      (dwq_ref, dwk_ref)[p // wide].at[pl.ds(pl.multiple_of(m * cols, cols), cols), pl.ds(p % wide, q - p)],
                                      o_sem.at[m % 2, i])
                for i, (p, q) in enumerate(zip(cuts, cuts[1:]))]

    def middle(j, _):
        for i in range(2):
            near(i, j).wait_recv()
            held_s[1 + i, j, (a, b)[i]] = (half_s[i, j] + near_s[i, j].astype(f32)).astype(bf)
            far(i, i, j).start()
            near(i, j).wait_send()
        for i in range(2):
            pair(2 + i, j).wait_send()
        for copy in inputs(j):
            copy.start()

    def inputs(j):
        return [pltpu.make_async_copy(ref.at[:, pl.ds(pl.multiple_of(j * cols, cols), cols)], pair_s.at[i, j], x_sem.at[i, j])
                for i, ref in enumerate((x_ref, dy_ref))]

    for copy in block(0):
        copy.start()

    def weight(m, _):
        @pl.when(m + 1 < TILES)
        def _():
            for copy in block(m + 1):
                copy.start()

        @pl.when(m == 2)
        def _():
            _loop(TILES, middle)

        @pl.when(m >= 2)
        def _():
            for copy in put(m - 2):
                copy.wait()

        for copy in block(m):
            copy.wait()
        t = jnp.concatenate([spot((m % 2) * depth + c)[...] for c in range(depth)], axis=1)
        for c in range(width):
            end = min((c + 1) * cols, 2 * wide)
            made(m, c)[:, : end - c * cols] = jnp.dot(t, g_s[:, c * cols : end], preferred_element_type=f32).astype(bf)
        for copy in put(m):
            copy.start()

    _loop(TILES, weight)

    lanes = [slice(l * HEAD, (l + 1) * HEAD) for l in range(cols // HEAD)]

    def at16(r):
        return pl.ds(pl.multiple_of(r * 16, 16), 16)

    def scales(r, _):
        at = at16(r)
        total = jnp.zeros((16, HEAD), f32)
        for j in range(TILES):
            t = pair_s[0, j, at, :].astype(f32)
            for l in lanes:
                total += t[:, l] * t[:, l]
        scale_s[at, :] = jnp.broadcast_to(lax.rsqrt(total.sum(-1, keepdims=True) * (1 / d) + 1e-6), (16, HEAD))
        mean_s[at, :] = jnp.zeros((16, HEAD), f32)

    for j in range(TILES):
        for copy in inputs(j):
            copy.wait()
    _loop(rows // 16, scales)

    for j in range(TILES):
        for i in range(2):
            for h in range(2):
                far(i, h, j).wait_recv()
        pair(3, j).wait_recv()
        gain = gain_ref[:, j * cols : (j + 1) * cols].astype(f32)
        norm_s[...] = jnp.zeros_like(norm_s)

        def gather(r, _):
            at = at16(r)
            g = own_s[j, at, :] + held_s[3, j, at, :].astype(f32) + far_s[0, j, at, :].astype(f32) + far_s[1, j, at, :].astype(f32)
            own_s[j, at, :] = g
            g = g * pair_s[0, j, at, :].astype(f32) * jnp.concatenate([scale_s[at, :]] * len(lanes), axis=1)
            norm_s[...] += g
            g = g * gain
            mean_s[at, :] += sum(g[:, l] for l in lanes)

        _loop(rows // 16, gather)
        gains_s[0, :, j * cols : (j + 1) * cols] = norm_s[...].sum(axis=0, keepdims=True)

    gains = [remote(gains_s.at[0], gains_s.at[1 + r], gain_send.at[r], gain_recv.at[r], who) for r, who in enumerate(others)]
    for copy in gains:
        copy.start()

    def derive(r, _):
        at = at16(r)
        scale = scale_s[at, :]
        mean = jnp.broadcast_to(mean_s[at, :].sum(-1, keepdims=True) * (1 / d), (16, HEAD)) * scale
        scale, mean = (jnp.concatenate([t] * len(lanes), axis=1) for t in (scale, mean))
        for j in range(TILES):
            by_x = scale * (own_s[j, at, :] * gain_ref[:, j * cols : (j + 1) * cols].astype(f32) - pair_s[0, j, at, :].astype(f32) * mean)
            pair_s[1, j, at, :] = (pair_s[1, j, at, :].astype(f32) + by_x.astype(bf).astype(f32)).astype(bf)

    _loop(rows // 16, derive)

    def results(j):
        return pltpu.make_async_copy(pair_s.at[1, j], dx_ref.at[:, pl.ds(pl.multiple_of(j * cols, cols), cols)], out_sem.at[j])

    _loop(TILES, lambda j, _: results(j).start())
    def close(j, _):
        for i in range(2):
            for h in range(2):
                far(i, h, j).wait_send()
        results(j).wait()

    _loop(TILES, close)
    for m in range(TILES - 2, TILES):
        for copy in put(m):
            copy.wait()
    for copy in gains:
        copy.wait()
    total = jnp.zeros((1, d), f32)
    for r in range(n):
        total += gains_s[lax.rem(me + n - r, n)]
    dgain_ref[...] = total


def finish(n, x, dy, gain, dq, dk, dv, wt, turned):
    rows, d = x.shape
    cols, half, wide = d // TILES, rows // 2, dq.shape[1]
    heads = wide // HEAD
    pieces = len({c * cols for c in range(-(-2 * wide // cols))} | {wide})
    f32, bf = jnp.float32, jnp.bfloat16
    anywhere, vmem = pl.BlockSpec(memory_space=pl.ANY), pl.BlockSpec(memory_space=pltpu.VMEM)
    weight = jax.ShapeDtypeStruct((d, wide), bf)
    return pl.pallas_call(
        functools.partial(_finish, n, heads),
        out_shape=[jax.ShapeDtypeStruct(x.shape, bf), jax.ShapeDtypeStruct((1, d), f32), weight, weight],
        in_specs=[anywhere, anywhere, vmem] + [anywhere] * 5,
        out_specs=[anywhere, vmem] + [anywhere] * 2,
        scratch_shapes=[pltpu.VMEM((n * rows, 3 * wide), bf), pltpu.VMEM(wt.shape, bf), pltpu.VMEM((2, TILES, rows, cols), bf),
                        pltpu.VMEM((4, TILES, rows, cols), bf), pltpu.VMEM((2, TILES, half, cols), bf), pltpu.VMEM((2, TILES, rows, cols), bf),
                        pltpu.VMEM((2, TILES, half, cols), f32), pltpu.VMEM((TILES, rows, cols), f32), pltpu.VMEM((AHEAD, rows, cols), f32),
                        pltpu.VMEM((16, cols), f32), pltpu.VMEM((rows, HEAD), f32), pltpu.VMEM((rows, HEAD), f32),
                        pltpu.VMEM((n, 1, d), f32), DMA((n, 3)), DMA((TILES,)), DMA((4, TILES)), DMA((4, TILES)), DMA((2, TILES)),
                        DMA((2, TILES)), DMA((2, 2, TILES)), DMA((2, 2, TILES)), DMA((n - 1,)), DMA((n - 1,)), DMA((2, n)), DMA((2, pieces)),
                        DMA((2, TILES)), DMA((TILES,))],
        compiler_params=pltpu.CompilerParams(collective_id=2, has_side_effects=True, vmem_limit_bytes=MOST),
        cost_estimate=pl.CostEstimate(flops=10 * n * rows * d * wide, transcendentals=0, bytes_accessed=6 * n * rows * d),
        name="finish",
    )(x, dy, gain[None], dq, dk, dv, wt, turned)


def _results(turned_ref, dv_ref, *refs):
    count = len(refs) // 2
    out_ref = refs[count]
    for a, b in zip(refs[:count], refs[count + 1 :]):
        b[...] = a[...]
    out_ref[...] = jnp.dot(turned_ref[...], dv_ref[...], preferred_element_type=jnp.float32).astype(jnp.bfloat16)


def results(turned, dv, dx, dgain, dwq, dwk):
    d, whole = turned.shape
    cols, wide = d // TILES, dv.shape[1]
    down = pl.BlockSpec((cols, wide), lambda j: (j, 0))

    def across(t):
        return pl.BlockSpec((t.shape[0], cols), lambda j: (0, j))

    others = [(dx, across(dx)), (dgain, across(dgain)), (dwq, down), (dwk, down)]
    dwv, *rest = pl.pallas_call(
        _results,
        grid=(TILES,),
        in_specs=[pl.BlockSpec((cols, whole), lambda j: (j, 0)), pl.BlockSpec(dv.shape, lambda j: (0, 0))] + [spec for _, spec in others],
        out_specs=[down] + [spec for _, spec in others],
        out_shape=[jax.ShapeDtypeStruct((d, wide), jnp.bfloat16)] + [jax.ShapeDtypeStruct(t.shape, t.dtype) for t, _ in others],
        compiler_params=pltpu.CompilerParams(dimension_semantics=("arbitrary",), vmem_limit_bytes=MOST),
        cost_estimate=pl.CostEstimate(flops=2 * d * whole * wide, transcendentals=0, bytes_accessed=2 * turned.size + 10 * d * wide),
        name="results",
    )(turned, dv, *[t for t, _ in others])
    return *rest, dwv


def solution(mesh):
    n = mesh.shape["tp"]

    def step(x, dy, gain, wq, wk, wv, wo):
        turned, q, k, v, early, wt, wot = project(n, x, dy, gain, wq, wk, wv, wo)
        d_seen, lse, delta, dwo = attend_gather(n, dy, early, q, k, v, wot)
        dq, dk, dv, dwo = attend_bwd(q, k, v, d_seen, lse, delta, dwo, min(512, q.shape[1]))
        dx, dgain, dwq, dwk = finish(n, x, dy, gain, dq, dk, dv, wt, turned)
        return *results(turned, dv, dx, dgain, dwq, dwk), dwo

    tokens, columns = P(("dp", "tp"), None), P(None, "tp")
    return jax.shard_map(
        step,
        mesh=mesh,
        in_specs=(tokens, tokens, P(None), columns, columns, columns, P("tp", None)),
        out_specs=(tokens, P("dp", None), P("dp", "tp"), P("dp", "tp"), P("dp", "tp"), P(("dp", "tp"), None)),
        check_vma=False,
    )
```
